32 devices in a mesh: gx: 2 (over x), gy: 4 (over y, core), gz: 4 (over z).
Axes of the slice: x: 2, y: 2, z: 4, core: 2. Of those that a mesh axis runs over, the one named last changes fastest.
Arguments:
- tokens: bfloat16 [1024, 4608], P('gx', 'gy'), may hold values from -6 to 6
- base_up_weight: bfloat16 [4608, 18432], P('gy', ('gz', 'gx')), may hold values from -0.09375 to 0.09375
- adapter_down_weight: bfloat16 [64, 16, 4608], P(None, None, 'gy'), may hold values from -0.09375 to 0.09375
- adapter_up_weight: bfloat16 [64, 16, 18432], P('gx', None, 'gz'), may hold values from -1.5 to 1.5
- block_adapter_index: int32 [8], P('gx'), may hold values from 0 to 63
- request_rows: int32 [8], P('gx'), may hold values from 1 to 128
Outputs:
- projected: bfloat16 [1024, 18432], P(('gx', 'gy'), 'gz')
The draws below stay inside these ranges and needn't reach their ends.
Inputs may be any that keep to these rules, and one draw needn't show every extreme that they name: `request_rows`: live rows of each block.
All inputs are finite; a program needn't handle non-finite values.
Results may differ from the reference program's by a relative error of at most 0.0047.
Values may be sent and summed in bfloat16 or wider, within the bound.
A program may use at most 128 MiB of HBM per device.

```python
import jax
import jax.numpy as jnp
from jax import lax

MODEL_WIDTH = 4608
HIDDEN_UNITS = 18432
ADAPTER_RANK = 16
ADAPTER_COUNT = 64
BLOCK = 128
BLOCKS = 8
ROWS = 1024


def touch_ends(array, rng, low, largest):
    place = [jax.random.randint(jax.random.fold_in(rng, axis), (), 0, length) for axis, length in enumerate(array.shape)]
    main_axis = array.shape.index(max(array.shape))
    beside = place[:main_axis] + [(place[main_axis] + 1) % array.shape[main_axis]] + place[main_axis + 1:]
    return array.at[tuple(place)].set(low).at[tuple(beside)].set(largest)


def block_scale(own_key, shape, pieces, least, high):
    factor_of = 1.0
    for axis_at, parts in pieces:
        steps = jax.random.uniform(jax.random.fold_in(jax.random.fold_in(own_key, 6), axis_at), (parts,), jnp.float32, least / len(pieces), high / len(pieces))
        factor_of = factor_of * jnp.repeat(jnp.exp(steps), shape[axis_at] // parts).reshape((-1,) + (1,) * (len(shape) - 1 - axis_at))
    return factor_of


def gaussian(key, dims, scale, most, shards=(), kind=jnp.bfloat16):
    values = scale * jax.random.normal(key, dims, jnp.float32)
    if shards:
        values = values * block_scale(key, dims, shards, -0.22, 0.18)
    return jnp.clip(values, -most, most).astype(kind)


def setup_inputs(seed: int = 0) -> dict:
    streams_of = jax.random.split(jax.random.key(seed), 7)
    return {
        "tokens": gaussian(streams_of[0], (ROWS, MODEL_WIDTH), 1.0, 6.0, ((0, 2), (1, 4))),
        "base_up_weight": gaussian(streams_of[1], (MODEL_WIDTH, HIDDEN_UNITS), MODEL_WIDTH ** -0.5, 0.09375, ((0, 4), (1, 8))),
        "adapter_down_weight": gaussian(streams_of[2], (ADAPTER_COUNT, ADAPTER_RANK, MODEL_WIDTH), MODEL_WIDTH ** -0.5, 0.09375, ((2, 4),)),
        "adapter_up_weight": gaussian(streams_of[3], (ADAPTER_COUNT, ADAPTER_RANK, HIDDEN_UNITS), ADAPTER_RANK ** -0.5, 1.5, ((0, 2), (2, 4))),
        "block_adapter_index": touch_ends(jax.random.randint(streams_of[4], (BLOCKS,), 0, ADAPTER_COUNT), jax.random.fold_in(streams_of[4], 1), 0, ADAPTER_COUNT - 1).astype(jnp.int32),
        "request_rows": touch_ends(jax.random.randint(streams_of[5], (BLOCKS,), 1, BLOCK + 1), jax.random.fold_in(streams_of[5], 1), 1, BLOCK).astype(jnp.int32),
    }


def reference(tokens, base_up_weight, adapter_down_weight, adapter_up_weight, block_adapter_index, request_rows):
    blocks = block_adapter_index.shape[0]
    tok_blocks = tokens.reshape(blocks, BLOCK, MODEL_WIDTH)

    def one_block(items):
        block_tokens, adapter_index, live_count = items
        down_factor = lax.dynamic_index_in_dim(adapter_down_weight, adapter_index, 0, keepdims=False)
        up_factor = lax.dynamic_index_in_dim(adapter_up_weight, adapter_index, 0, keepdims=False)
        shrink = jnp.dot(block_tokens, down_factor.T, preferred_element_type=jnp.float32)
        shrink_low = shrink.astype(jnp.bfloat16)
        expand = jnp.dot(shrink_low, up_factor, preferred_element_type=jnp.float32)
        base = jnp.dot(block_tokens, base_up_weight, preferred_element_type=jnp.float32)
        live_mask = jnp.arange(BLOCK, dtype=jnp.int32) < live_count
        return jnp.where(live_mask[:, None], base + 2.0 * expand, 0.0).astype(jnp.bfloat16)

    result = lax.map(one_block, (tok_blocks, block_adapter_index, request_rows))
    return result.reshape(blocks * BLOCK, HIDDEN_UNITS)
```

```python
import functools

import jax
import jax.numpy as jnp
from jax import lax
from jax.experimental import pallas as pl
from jax.experimental.pallas import tpu as pltpu
from jax.sharding import PartitionSpec as P

F32 = jnp.float32
BF16 = jnp.bfloat16
STAGES = 4
FAR_PARTS = 3
MESH = pl.DeviceIdType.MESH


def general_body(
    tokens,
    base_up_weight,
    adapter_down_weight,
    adapter_up_weight,
    block_adapter_index,
    request_rows,
):
    rows, shard_width = tokens.shape
    groups = lax.axis_size("gy")
    blocks = block_adapter_index.shape[0]
    block = rows // blocks
    own_blocks = blocks // groups
    own_rows = own_blocks * block
    first = lax.axis_index("gy") * own_blocks
    count, rank_values, _ = adapter_down_weight.shape
    catalog = jnp.arange(count, dtype=jnp.int32)
    selected_adapters = (block_adapter_index[:, None] == catalog[None, :]).astype(BF16)
    chosen_down = jnp.dot(
        selected_adapters,
        adapter_down_weight.reshape(count, rank_values * shard_width),
        preferred_element_type=F32,
    )
    chosen_down = chosen_down.astype(BF16).reshape(blocks, rank_values, shard_width)
    tok_blocks = tokens.reshape(blocks, block, shard_width)
    shrink_part = jnp.einsum("bmd,brd->bmr", tok_blocks, chosen_down, preferred_element_type=F32)
    shrink_own = lax.psum_scatter(shrink_part, "gy", scatter_dimension=0, tiled=True)
    shrink_low = shrink_own.astype(BF16)
    adapter_factors = lax.all_gather(adapter_up_weight, "gx", axis=0, tiled=True)
    out_width = adapter_factors.shape[2]
    own_picks = lax.dynamic_slice_in_dim(selected_adapters, first, own_blocks, 0)
    chosen_up = jnp.dot(
        own_picks,
        adapter_factors.reshape(count, rank_values * out_width),
        preferred_element_type=F32,
    )
    chosen_up = chosen_up.astype(BF16).reshape(own_blocks, rank_values, out_width)
    expand = jnp.einsum("bmr,brf->bmf", shrink_low, chosen_up, preferred_element_type=F32)
    expand = expand.reshape(own_rows, out_width)
    partial_value = jnp.dot(
        tokens,
        lax.all_gather(base_up_weight, "gx", axis=1, tiled=True),
        preferred_element_type=F32,
    )
    extra = 2.0 * expand
    total = lax.psum_scatter(partial_value, "gy", scatter_dimension=0, tiled=True) + extra
    own_live = lax.dynamic_slice_in_dim(request_rows, first, own_blocks, 0)
    live_mask = (jnp.arange(block, dtype=jnp.int32)[None, :] < own_live[:, None]).reshape(
        own_rows, 1
    )
    return jnp.where(live_mask, total, 0.0).astype(BF16)


def kernel(
    near_spans,
    far_spans,
    index_hbm,
    live_hbm,
    tok_hbm,
    w_hbm,
    down_hbm,
    up_hbm,
    out_ref,
    index_ref,
    live_ref,
    tok,
    far_tok,
    w,
    down,
    up,
    name_send,
    name_in,
    up_own,
    up_send,
    up_in,
    up_peer,
    shrink_own,
    shrink_send,
    shrink_in,
    low_send,
    low_in,
    far_extra,
    peer_extra,
    a_send,
    a_in,
    keep,
    fa_send,
    fa_in,
    fkeep,
    b_send,
    b_in,
    fb_send,
    fb_in,
    c_send,
    c_in,
    load_sem,
    w_sem,
    a_sem,
    fa_sem,
    b_sem,
    fb_sem,
    c_sem,
    x_sem,
    z_sem,
    shrink_sem,
    name_sem,
    low_sem,
    up_sem,
):
    gx = lax.axis_index("gx")
    gy = lax.axis_index("gy")
    gz = lax.axis_index("gz")
    core = lax.rem(gy, 2)
    yy = lax.div(gy, 2)
    y_far = 1 - yy
    zp = lax.rem(gz, 2)
    x_peer = {"gx": 1 - gx}
    core_peer = {"gy": gy + 1 - 2 * core}
    y_peer = {"gy": lax.rem(gy + 2, 4)}
    diagonal = {"gy": 3 - gy}
    z_peer = {"gz": gz + 1 - 2 * zp}
    block = out_ref.shape[0]
    cols = w.shape[1]
    held, ranks, _ = up.shape
    part_rows = block // STAGES
    near = len(near_spans)
    far = len(far_spans)

    def remote(src, dst, sems, n, device):
        return pltpu.make_async_remote_copy(
            src_ref=src,
            dst_ref=dst,
            send_sem=sems.at[0],
            recv_sem=sems.at[1 + n],
            device_id=device,
            device_id_type=MESH,
        )

    def rows_at(block_at, first, count):
        return pl.ds(pl.multiple_of(block_at * block + first, count), count)

    def load(src, dst, sem):
        copy = pltpu.make_async_copy(src, dst, sem)
        copy.start()
        return copy

    def tok_half(y_at, n):
        span = pl.ds(pl.multiple_of(y_at * 2 * block, 2 * block), 2 * block)
        return load(tok_hbm.at[span, :], tok.at[span, :], load_sem.at[n])

    def w_load(n):
        start, width = near_spans[n]
        span = pl.ds(start, width)
        return load(w_hbm.at[:, span], w.at[:, span], w_sem.at[n])

    tok_far_load = tok_half(y_far, 0)
    w_loads = [w_load(0)]
    tok_own_load = tok_half(yy, 1)
    index_load = load(index_hbm, index_ref, load_sem.at[2])
    live_load = load(live_hbm, live_ref, load_sem.at[3])
    w_loads += [w_load(n) for n in range(1, 3)]
    down_load = load(down_hbm, down, load_sem.at[4])
    w_loads += [w_load(n) for n in range(3, near)]
    up_load = load(up_hbm, up, load_sem.at[5])

    barrier = pltpu.get_barrier_semaphore()
    for device in (x_peer, core_peer, y_peer, diagonal, z_peer):
        pl.semaphore_signal(barrier, inc=1, device_id=device, device_id_type=MESH)

    def go(copy):
        copy.start()
        return copy

    x_copies, z_copies = [], []
    for r in range(STAGES):
        for y_at in (y_far, yy):
            n = len(x_copies)
            span = rows_at(2 * y_at + zp, r * part_rows, part_rows)
            x_copies.append(remote(tok.at[span, :], far_tok.at[span, :], x_sem, n, x_peer))
            z_copies.append(
                remote(far_tok.at[span, :], far_tok.at[span, :], z_sem, n, z_peer)
            )

    def relay(n):
        x_copies[n].wait_recv()
        go(z_copies[n])

    a_copies, fa_copies, b_copies, fb_copies, c_copies = {}, {}, {}, {}, {}

    def near_dot(u, n):
        y_at = (y_far, yy)[u]
        start, width = near_spans[n]
        lhs = jnp.concatenate(
            [
                tok[rows_at(2 * y_at + 1 - core, 0, block), :],
                tok[rows_at(2 * y_at + core, 0, block), :],
            ],
            axis=0,
        )
        span = slice(start, start + width)
        part = jnp.dot(lhs, w[:, span], preferred_element_type=F32)
        a_send[u, :, span] = part[:block]
        keep[u, :, span] = part[block:]

    def near_give(u, n):
        start, width = near_spans[n]
        span = pl.ds(start, width)
        a_copies[u, n] = go(
            remote(
                a_send.at[u, :, span], a_in.at[u, :, span], a_sem, u * near + n, core_peer
            )
        )

    def near_pair(n, hold=False):
        start, width = near_spans[n]
        span = pl.ds(start, width)
        a_copies[0, n].wait_recv()
        b_send[:, span] = (keep[0, :, span] + a_in[0, :, span]).astype(BF16)
        b_copies[n] = remote(b_send.at[:, span], b_in.at[:, span], b_sem, n, y_peer)
        if not hold:
            go(b_copies[n])

    def far_dot(h, n):
        start, width = far_spans[n]
        lhs = jnp.concatenate(
            [
                far_tok[rows_at(2 * y_at + c, h * part_rows, part_rows), :]
                for c in (1 - core, core)
                for y_at in (y_far, yy)
            ],
            axis=0,
        )
        span = slice(start, start + width)
        part = jnp.dot(lhs, w[:, span], preferred_element_type=F32)
        fa_send[h, :, span] = part[: 2 * part_rows]
        fkeep[h, :, span] = part[2 * part_rows :]
        span = pl.ds(start, width)
        fa_copies[h, n] = go(
            remote(
                fa_send.at[h, :, span], fa_in.at[h, :, span], fa_sem, h * far + n, core_peer
            )
        )

    def far_pair(h, n):
        start, width = far_spans[n]
        span = pl.ds(start, width)
        fa_copies[h, n].wait_recv()
        out_rows = pl.ds(0, part_rows)
        fb_send[h, :, span] = (fkeep[h, out_rows, span] + fa_in[h, out_rows, span]).astype(
            BF16
        )
        fb_copies[h, n] = go(
            remote(fb_send.at[h, :, span], fb_in.at[h, :, span], fb_sem, h * far + n, y_peer)
        )

    def far_return(h, n):
        start, width = far_spans[n]
        span = pl.ds(start, width)
        own_rows = pl.ds(part_rows, part_rows)
        fb_copies[h, n].wait_recv()
        total = fkeep[h, own_rows, span] + fa_in[h, own_rows, span]
        total += fb_in[h, :, span].astype(F32)
        total += peer_extra[pl.ds(h * part_rows, part_rows), span]
        c_send[h, :, span] = total.astype(BF16)
        c_copies[h, n] = go(
            remote(c_send.at[h, :, span], c_in.at[h, :, span], c_sem, h * far + n, x_peer)
        )

    def expanded(low, factor):
        return 2.0 * lax.dot_general(
            low, factor, (((0,), (0,)), ((), ())), preferred_element_type=F32
        )

    def live_rows(first, count):
        at = lax.broadcasted_iota(jnp.int32, (count, 1), 0) + first
        return at < live_ref[gy]

    def out_span(side, start, width):
        return pl.ds(pl.multiple_of(side * cols + start, 128), width)

    def finish_near(n):
        start, width = near_spans[n]
        span = pl.ds(start, width)
        a_copies[1, n].wait_recv()
        b_copies[n].wait_recv()
        total = keep[1, :, span] + a_in[1, :, span] + b_in[:, span].astype(F32)
        factor = up_own[:, out_span(gx, start, width)] + up_in[:, span]
        total += expanded(low_send[...], factor)
        out_ref[:, out_span(gx, start, width)] = jnp.where(
            live_rows(0, block), total, 0.0
        ).astype(BF16)

    def finish_far(h, n):
        start, width = far_spans[n]
        span = pl.ds(start, width)
        c_copies[h, n].wait_recv()
        rows = pl.ds(h * part_rows, part_rows)
        total = c_in[h, :, span].astype(F32) + far_extra[rows, span]
        out_ref[rows, out_span(1 - gx, start, width)] = jnp.where(
            live_rows(h * part_rows, part_rows), total, 0.0
        ).astype(BF16)

    def near_step(u, n):
        if u == 0:
            w_loads[n].wait()
        near_dot(u, n)
        near_give(u, n)

    tok_far_load.wait()
    w_loads[0].wait()
    near_dot(0, 0)
    tok_own_load.wait()
    index_load.wait()
    live_load.wait()
    name_send[...] = jnp.full(name_send.shape, index_ref[gy].astype(F32))
    pl.semaphore_wait(barrier, 5)
    near_give(0, 0)
    name_copy = go(remote(name_send, name_in, name_sem, 0, x_peer))
    early = len(x_copies) - 2
    for n in range(early):
        go(x_copies[n])

    shrink_copies = []

    def shrink_part(at):
        return lax.dot_general(
            down[index_ref[at]],
            tok[rows_at(at, 0, block), :],
            (((1,), (1,)), ((), ())),
            preferred_element_type=F32,
        )

    def shrink_give(d, device):
        shrink_send[d] = shrink_part(device["gy"])
        shrink_copies.append(
            go(remote(shrink_send.at[d], shrink_in.at[d], shrink_sem, d, device))
        )

    near_step(0, 1)
    near_step(0, 2)
    near_pair(0)
    down_load.wait()
    shrink_give(0, y_peer)
    shrink_give(1, diagonal)
    near_pair(1)
    near_step(0, 3)
    shrink_give(2, core_peer)
    near_pair(2)
    for n in range(4, near):
        near_step(0, n)
    shrink_own[...] = shrink_part(gy)
    for n in range(3, near - 1):
        near_pair(n)
    relay(0)
    near_pair(near - 1, hold=True)

    up_load.wait()
    slot = index_ref[gy] - gx * held
    mine = up[jnp.clip(slot, 0, held - 1)]
    here = jnp.logical_and(slot >= 0, slot < held)
    up_own[...] = jnp.where(here, mine, jnp.zeros_like(mine))
    name_copy.wait_recv()
    rank_at = lax.broadcasted_iota(jnp.int32, (ranks, held * ranks), 0)
    slot_at = lax.broadcasted_iota(jnp.int32, (ranks, held * ranks), 1) + gx * held * ranks
    wanted = name_in[0:1, 0:1] * float(ranks)
    hit = (slot_at - rank_at).astype(F32) == wanted
    pick = jnp.where(hit, 1.0, 0.0).astype(BF16)

    def picked(side, start, width):
        factors = up[:, :, out_span(side, start, width)].reshape(held * ranks, width)
        return jnp.dot(pick, factors, preferred_element_type=F32).astype(BF16)

    for start, width in far_spans:
        up_send[:, pl.ds(start, width)] = picked(1 - gx, start, width)
    for copy in shrink_copies:
        copy.wait_recv()
    shrink = (shrink_own[...] + shrink_in[0]) + (shrink_in[1] + shrink_in[2])
    low_send[...] = shrink.astype(BF16)
    low_copy = go(remote(low_send, low_in, low_sem, 0, x_peer))
    for n in range(early, len(x_copies)):
        go(x_copies[n])
    up_copy = go(remote(up_send, up_in, up_sem, 0, x_peer))
    near_step(1, 0)
    near_step(1, 1)
    relay(1)
    for start, width in far_spans:
        up_peer[:, pl.ds(start, width)] = picked(gx, start, width)
    near_step(1, 2)
    relay(2)
    for n in range(3, near):
        near_step(1, n)

    relay(3)

    def far_tokens(h):
        z_copies[2 * h].wait_recv()
        z_copies[2 * h + 1].wait_recv()

    far_tokens(0)
    for n in range(far):
        far_dot(0, n)
    relay(4)
    for start, width in far_spans:
        far_extra[:, pl.ds(start, width)] = expanded(
            low_send[...], up_own[:, out_span(1 - gx, start, width)]
        )
    for n in range(far):
        far_pair(0, n)
    relay(5)
    far_tokens(1)
    for n in range(far):
        far_dot(1, n)
    relay(6)
    low_copy.wait_recv()
    for start, width in far_spans:
        span = pl.ds(start, width)
        peer_extra[:, span] = expanded(low_in[...], up_peer[:, span])
    for n in range(far):
        far_pair(1, n)
    relay(7)
    far_tokens(2)
    far_dot(2, 0)
    far_return(0, 0)
    far_dot(2, 1)
    far_dot(2, 2)
    far_return(0, 1)
    far_pair(2, 0)
    far_pair(2, 1)
    far_return(0, 2)
    far_pair(2, 2)
    far_tokens(3)
    far_dot(3, 0)
    far_return(1, 0)
    far_dot(3, 1)
    far_dot(3, 2)
    far_return(1, 1)
    for n in range(far):
        far_pair(3, n)
    go(b_copies[near - 1])
    far_return(1, 2)
    up_copy.wait_recv()
    for n in range(0, near - 1):
        finish_near(n)
    for n in range(far):
        far_return(2, n)
    for n in range(far):
        finish_far(0, n)
    for n in range(far):
        finish_far(1, n)
    for n in range(far):
        far_return(3, n)
    for n in range(far):
        finish_far(2, n)
    finish_near(near - 1)
    for n in range(far):
        finish_far(3, n)

    half = pl.ds(0, 2 * block)
    for src, sems in (
        (a_send, a_sem),
        (fa_send, fa_sem),
        (b_send, b_sem),
        (fb_send, fb_sem),
        (c_send, c_sem),
        (tok.at[half, :], x_sem),
        (tok.at[half, :], z_sem),
        (shrink_send, shrink_sem),
        (name_send, name_sem),
        (low_send, low_sem),
        (up_send, up_sem),
    ):
        remote(src, src, sems, 0, x_peer).wait_send()


def spans_of(cols, first, wide):
    spans, start = [], 0
    while start < cols:
        width = min(wide if start else first, cols - start)
        spans.append((start, width))
        start += width
    return spans


def fused_body(
    tokens,
    base_up_weight,
    adapter_down_weight,
    adapter_up_weight,
    block_adapter_index,
    request_rows,
):
    rows, depth = tokens.shape
    cols = base_up_weight.shape[1]
    blocks = block_adapter_index.shape[0]
    block = rows // blocks
    count, ranks, _ = adapter_down_weight.shape
    held, _, out_width = adapter_up_weight.shape
    near_spans = spans_of(cols, 256, 512)
    far_spans = spans_of(cols, cols // FAR_PARTS, cols // FAR_PARTS)
    near, far = len(near_spans), len(far_spans)
    part_rows = block // STAGES
    in_hbm = pl.BlockSpec(memory_space=pltpu.HBM)

    def dma(n):
        return pltpu.SemaphoreType.DMA((1 + n,))

    return pl.pallas_call(
        functools.partial(kernel, near_spans, far_spans),
        out_shape=pltpu.VMEM((block, out_width), BF16),
        in_specs=[in_hbm] * 6,
        out_specs=pl.BlockSpec(memory_space=pltpu.VMEM),
        scratch_shapes=[
            pltpu.SMEM((blocks,), jnp.int32),
            pltpu.SMEM((blocks,), jnp.int32),
            pltpu.VMEM((rows, depth), BF16),
            pltpu.VMEM((rows, depth), BF16),
            pltpu.VMEM((depth, cols), BF16),
            pltpu.VMEM((count, ranks, depth), BF16),
            pltpu.VMEM((held, ranks, out_width), BF16),
            pltpu.VMEM((8, 128), F32),
            pltpu.VMEM((8, 128), F32),
            pltpu.VMEM((ranks, out_width), BF16),
            pltpu.VMEM((ranks, cols), BF16),
            pltpu.VMEM((ranks, cols), BF16),
            pltpu.VMEM((ranks, cols), BF16),
            pltpu.VMEM((ranks, block), F32),
            pltpu.VMEM((3, ranks, block), F32),
            pltpu.VMEM((3, ranks, block), F32),
            pltpu.VMEM((ranks, block), BF16),
            pltpu.VMEM((ranks, block), BF16),
            pltpu.VMEM((block, cols), F32),
            pltpu.VMEM((block, cols), F32),
            pltpu.VMEM((2, block, cols), F32),
            pltpu.VMEM((2, block, cols), F32),
            pltpu.VMEM((2, block, cols), F32),
            pltpu.VMEM((STAGES, 2 * part_rows, cols), F32),
            pltpu.VMEM((STAGES, 2 * part_rows, cols), F32),
            pltpu.VMEM((STAGES, 2 * part_rows, cols), F32),
            pltpu.VMEM((block, cols), BF16),
            pltpu.VMEM((block, cols), BF16),
            pltpu.VMEM((STAGES, part_rows, cols), BF16),
            pltpu.VMEM((STAGES, part_rows, cols), BF16),
            pltpu.VMEM((STAGES, part_rows, cols), BF16),
            pltpu.VMEM((STAGES, part_rows, cols), BF16),
            pltpu.SemaphoreType.DMA((6,)),
            pltpu.SemaphoreType.DMA((near,)),
            dma(2 * near),
            dma(STAGES * far),
            dma(near),
            dma(STAGES * far),
            dma(STAGES * far),
            dma(2 * STAGES),
            dma(2 * STAGES),
            dma(3),
            dma(1),
            dma(1),
            dma(1),
        ],
        compiler_params=pltpu.CompilerParams(
            collective_id=0, has_side_effects=True, vmem_limit_bytes=56 * 1024 * 1024
        ),
    )(
        block_adapter_index,
        request_rows,
        tokens,
        base_up_weight,
        adapter_down_weight,
        adapter_up_weight,
    )


def solution(mesh):
    in_specs = (
        P("gx", "gy"),
        P("gy", ("gz", "gx")),
        P(None, None, "gy"),
        P("gx", None, "gz"),
        P("gx"),
        P("gx"),
    )
    out_specs = P(("gx", "gy"), "gz")
    sizes = mesh.shape

    def body(*arrays):
        blocks = arrays[4].shape[0]
        paired = sizes["gx"] == 2 and sizes["gy"] == 4 and sizes["gz"] % 2 == 0
        cols = arrays[1].shape[1]
        cut = cols % (FAR_PARTS * 128) == 0 and len(spans_of(cols, 256, 512)) > 4
        cut = cut and arrays[0].shape[0] // blocks % (STAGES * 16) == 0
        if paired and cut and blocks == sizes["gy"]:
            return fused_body(*arrays)
        return general_body(*arrays)

    return jax.shard_map(body, mesh=mesh, in_specs=in_specs, out_specs=out_specs, check_vma=False)
```

```python
import functools

import jax
import jax.numpy as jnp
from jax import lax
from jax.experimental import pallas as pl
from jax.experimental.pallas import tpu as pltpu
from jax.sharding import PartitionSpec as P

F32 = jnp.float32
BF16 = jnp.bfloat16
STAGES = 4
CUTS = 2
NEAR = (2, 4, 4, 3, 5)
FAR = (6, 8, 4)
MESH = pl.DeviceIdType.MESH


def general_body(
    tokens,
    base_up_weight,
    adapter_down_weight,
    adapter_up_weight,
    block_adapter_index,
    request_rows,
):
    rows, shard_width = tokens.shape
    groups = lax.axis_size("gy")
    blocks = block_adapter_index.shape[0]
    block = rows // blocks
    own_blocks = blocks // groups
    own_rows = own_blocks * block
    first = lax.axis_index("gy") * own_blocks
    count, rank_values, _ = adapter_down_weight.shape
    catalog = jnp.arange(count, dtype=jnp.int32)
    selected_adapters = (block_adapter_index[:, None] == catalog[None, :]).astype(BF16)
    chosen_down = jnp.dot(
        selected_adapters,
        adapter_down_weight.reshape(count, rank_values * shard_width),
        preferred_element_type=F32,
    )
    chosen_down = chosen_down.astype(BF16).reshape(blocks, rank_values, shard_width)
    tok_blocks = tokens.reshape(blocks, block, shard_width)
    shrink_part = jnp.einsum("bmd,brd->bmr", tok_blocks, chosen_down, preferred_element_type=F32)
    shrink_own = lax.psum_scatter(shrink_part, "gy", scatter_dimension=0, tiled=True)
    shrink_low = shrink_own.astype(BF16)
    adapter_factors = lax.all_gather(adapter_up_weight, "gx", axis=0, tiled=True)
    out_width = adapter_factors.shape[2]
    own_picks = lax.dynamic_slice_in_dim(selected_adapters, first, own_blocks, 0)
    chosen_up = jnp.dot(
        own_picks,
        adapter_factors.reshape(count, rank_values * out_width),
        preferred_element_type=F32,
    )
    chosen_up = chosen_up.astype(BF16).reshape(own_blocks, rank_values, out_width)
    expand = jnp.einsum("bmr,brf->bmf", shrink_low, chosen_up, preferred_element_type=F32)
    expand = expand.reshape(own_rows, out_width)
    partial_value = jnp.dot(
        tokens,
        lax.all_gather(base_up_weight, "gx", axis=1, tiled=True),
        preferred_element_type=F32,
    )
    extra = 2.0 * expand
    total = lax.psum_scatter(partial_value, "gy", scatter_dimension=0, tiled=True) + extra
    own_live = lax.dynamic_slice_in_dim(request_rows, first, own_blocks, 0)
    live_mask = (jnp.arange(block, dtype=jnp.int32)[None, :] < own_live[:, None]).reshape(
        own_rows, 1
    )
    return jnp.where(live_mask, total, 0.0).astype(BF16)


def kernel(
    near_spans,
    far_spans,
    index_hbm,
    live_hbm,
    tok_hbm,
    w_hbm,
    down_hbm,
    up_hbm,
    out_ref,
    index_ref,
    live_ref,
    tok,
    far_tok,
    w,
    down,
    up,
    name_send,
    name_in,
    up_own,
    up_send,
    up_in,
    up_peer,
    shrink_own,
    shrink_send,
    shrink_in,
    low_send,
    low_in,
    far_extra,
    peer_extra,
    a_send,
    a_in,
    keep,
    fa_send,
    fa_in,
    fkeep,
    b_send,
    b_in,
    fb_send,
    fb_in,
    c_send,
    c_in,
    load_sem,
    w_sem,
    send_sem,
    a_sem,
    fa_sem,
    b_sem,
    fb_sem,
    c_sem,
    x_sem,
    z_sem,
    shrink_sem,
    name_sem,
    low_sem,
    up_sem,
):
    gx = lax.axis_index("gx")
    gy = lax.axis_index("gy")
    gz = lax.axis_index("gz")
    core = lax.rem(gy, 2)
    yy = lax.div(gy, 2)
    y_far = 1 - yy
    zp = lax.rem(gz, 2)
    x_peer = {"gx": 1 - gx}
    core_peer = {"gy": gy + 1 - 2 * core}
    y_peer = {"gy": lax.rem(gy + 2, 4)}
    diagonal = {"gy": 3 - gy}
    z_peer = {"gz": gz + 1 - 2 * zp}
    block = out_ref.shape[0]
    cols = w.shape[1]
    held, ranks, _ = up.shape
    part_rows = block // STAGES
    piece = part_rows // CUTS
    near = len(near_spans)
    far = len(far_spans)

    def remote(src, dst, sent, sem, device):
        return pltpu.make_async_remote_copy(
            src_ref=src,
            dst_ref=dst,
            send_sem=send_sem.at[sent],
            recv_sem=sem,
            device_id=device,
            device_id_type=MESH,
        )

    def rows_at(block_at, first, count):
        return pl.ds(pl.multiple_of(block_at * block + first, count), count)

    def load(src, dst, sem):
        copy = pltpu.make_async_copy(src, dst, sem)
        copy.start()
        return copy

    def tok_half(y_at, n):
        span = pl.ds(pl.multiple_of(y_at * 2 * block, 2 * block), 2 * block)
        return load(tok_hbm.at[span, :], tok.at[span, :], load_sem.at[n])

    def w_load(n):
        start, width = near_spans[n]
        span = pl.ds(start, width)
        return load(w_hbm.at[:, span], w.at[:, span], w_sem.at[n])

    tok_far_load = tok_half(y_far, 0)
    w_loads = [w_load(0)]
    tok_own_load = tok_half(yy, 1)
    index_load = load(index_hbm, index_ref, load_sem.at[2])
    live_load = load(live_hbm, live_ref, load_sem.at[3])
    w_loads += [w_load(n) for n in range(1, 3)]
    down_load = load(down_hbm, down, load_sem.at[4])
    w_loads += [w_load(n) for n in range(3, near)]

    barrier = pltpu.get_barrier_semaphore()
    for device in (x_peer, core_peer, y_peer, diagonal, z_peer):
        pl.semaphore_signal(barrier, inc=1, device_id=device, device_id_type=MESH)

    def go(copy):
        copy.start()
        return copy

    x_copies, z_copies = [], []
    for h in range(STAGES):
        for r in range(CUTS):
            for y_at in (y_far, yy):
                span = rows_at(2 * y_at + zp, h * part_rows + r * piece, piece)
                x_copies.append(
                    remote(
                        tok.at[span, :],
                        far_tok.at[span, :],
                        2,
                        x_sem.at[len(x_copies)],
                        x_peer,
                    )
                )
                z_copies.append(
                    remote(far_tok.at[span, :], far_tok.at[span, :], 2, z_sem.at[h], z_peer)
                )

    def relay(n):
        x_copies[n].wait_recv()
        go(z_copies[n])

    a_copies, fa_copies, b_copies, fb_copies, c_copies = {}, {}, {}, {}, {}

    def near_dot(u, n):
        y_at = (y_far, yy)[u]
        start, width = near_spans[n]
        lhs = jnp.concatenate(
            [
                tok[rows_at(2 * y_at + 1 - core, 0, block), :],
                tok[rows_at(2 * y_at + core, 0, block), :],
            ],
            axis=0,
        )
        span = slice(start, start + width)
        part = jnp.dot(lhs, w[:, span], preferred_element_type=F32)
        a_send[u, :, span] = part[:block]
        keep[u, :, span] = part[block:]

    def near_give(u, n):
        start, width = near_spans[n]
        span = pl.ds(start, width)
        a_copies[u, n] = go(
            remote(
                a_send.at[u, :, span],
                a_in.at[u, :, span],
                0,
                a_sem.at[near if u else n],
                core_peer,
            )
        )

    def near_pair(n, hold=False):
        start, width = near_spans[n]
        span = pl.ds(start, width)
        a_copies[0, n].wait_recv()
        b_send[:, span] = (keep[0, :, span] + a_in[0, :, span]).astype(BF16)
        b_copies[n] = remote(b_send.at[:, span], b_in.at[:, span], 1, b_sem.at[n], y_peer)
        if not hold:
            go(b_copies[n])

    def far_dot(h, n):
        start, width = far_spans[n]
        lhs = jnp.concatenate(
            [
                far_tok[rows_at(2 * y_at + c, h * part_rows, part_rows), :]
                for c in (1 - core, core)
                for y_at in (y_far, yy)
            ],
            axis=0,
        )
        span = slice(start, start + width)
        part = jnp.dot(lhs, w[:, span], preferred_element_type=F32)
        fa_send[h, :, span] = part[: 2 * part_rows]
        fkeep[h, :, span] = part[2 * part_rows :]
        span = pl.ds(start, width)
        fa_copies[h, n] = go(
            remote(
                fa_send.at[h, :, span],
                fa_in.at[h, :, span],
                0,
                fa_sem.at[h % 2 * far + n],
                core_peer,
            )
        )

    def far_pair(h, n):
        start, width = far_spans[n]
        span = pl.ds(start, width)
        fa_copies[h, n].wait_recv()
        out_rows = pl.ds(0, part_rows)
        fb_send[h, :, span] = (fkeep[h, out_rows, span] + fa_in[h, out_rows, span]).astype(
            BF16
        )
        fb_copies[h, n] = go(
            remote(
                fb_send.at[h, :, span],
                fb_in.at[h, :, span],
                1,
                fb_sem.at[h * far + n],
                y_peer,
            )
        )

    def far_return(h, n):
        start, width = far_spans[n]
        span = pl.ds(start, width)
        own_rows = pl.ds(part_rows, part_rows)
        fb_copies[h, n].wait_recv()
        total = fkeep[h, own_rows, span] + fa_in[h, own_rows, span]
        total += fb_in[h, :, span].astype(F32)
        total += peer_extra[pl.ds(h * part_rows, part_rows), span]
        c_send[h, :, span] = total.astype(BF16)
        c_copies[h, n] = go(
            remote(
                c_send.at[h, :, span],
                c_in.at[h, :, span],
                1,
                c_sem.at[h + n if h == STAGES - 1 else h],
                x_peer,
            )
        )

    def expanded(low, factor):
        return 2.0 * lax.dot_general(
            low, factor, (((0,), (0,)), ((), ())), preferred_element_type=F32
        )

    def live_rows(first, count):
        at = lax.broadcasted_iota(jnp.int32, (count, 1), 0) + first
        return at < live_ref[gy]

    def out_span(side, start, width):
        return pl.ds(pl.multiple_of(side * cols + start, 128), width)

    def finish_near(n):
        start, width = near_spans[n]
        span = pl.ds(start, width)
        b_copies[n].wait_recv()
        total = keep[1, :, span] + a_in[1, :, span] + b_in[:, span].astype(F32)
        factor = up_own[:, out_span(gx, start, width)] + up_in[:, span]
        total += expanded(low_send[...], factor)
        out_ref[:, out_span(gx, start, width)] = jnp.where(
            live_rows(0, block), total, 0.0
        ).astype(BF16)

    def finish_far(h, n):
        start, width = far_spans[n]
        span = pl.ds(start, width)
        if h == STAGES - 1:
            c_copies[h, n].wait_recv()
        elif n == 0:
            remote(c_send.at[h], c_in.at[h], 1, c_sem.at[h], x_peer).wait_recv()
        rows = pl.ds(h * part_rows, part_rows)
        total = c_in[h, :, span].astype(F32) + far_extra[rows, span]
        out_ref[rows, out_span(1 - gx, start, width)] = jnp.where(
            live_rows(h * part_rows, part_rows), total, 0.0
        ).astype(BF16)

    def near_step(u, n):
        if u == 0:
            w_loads[n].wait()
        near_dot(u, n)
        near_give(u, n)

    tok_far_load.wait()
    w_loads[0].wait()
    near_dot(0, 0)
    tok_own_load.wait()
    pl.semaphore_wait(barrier, 5)
    early = len(x_copies) // 2
    for n in range(2):
        go(x_copies[n])
    index_load.wait()
    live_load.wait()
    name_send[...] = jnp.full(name_send.shape, index_ref[gy].astype(F32))
    name_copy = go(remote(name_send, name_in, 3, name_sem, x_peer))
    for n in range(2, early):
        go(x_copies[n])
    near_give(0, 0)

    shrink_copies = []

    def shrink_part(at):
        return lax.dot_general(
            down[index_ref[at]],
            tok[rows_at(at, 0, block), :],
            (((1,), (1,)), ((), ())),
            preferred_element_type=F32,
        )

    def shrink_give(d, device):
        shrink_send[d] = shrink_part(device["gy"])
        shrink_copies.append(
            go(remote(shrink_send.at[d], shrink_in.at[d], 3, shrink_sem, device))
        )

    near_step(0, 1)
    up_load = load(up_hbm, up, load_sem.at[5])
    near_step(0, 2)
    near_pair(0)
    down_load.wait()
    shrink_give(0, y_peer)
    shrink_give(1, diagonal)
    near_pair(1)
    near_step(0, 3)
    shrink_give(2, core_peer)
    near_pair(2)
    near_step(0, 4)
    relay(0)
    shrink_own[...] = shrink_part(gy)
    near_pair(3)
    relay(1)

    up_load.wait()
    slot = index_ref[gy] - gx * held
    mine = up[jnp.clip(slot, 0, held - 1)]
    here = jnp.logical_and(slot >= 0, slot < held)
    up_own[...] = jnp.where(here, mine, jnp.zeros_like(mine))
    name_copy.wait_recv()
    rank_at = lax.broadcasted_iota(jnp.int32, (ranks, held * ranks), 0)
    slot_at = lax.broadcasted_iota(jnp.int32, (ranks, held * ranks), 1) + gx * held * ranks
    wanted = name_in[0:1, 0:1] * float(ranks)
    hit = (slot_at - rank_at).astype(F32) == wanted
    pick = jnp.where(hit, 1.0, 0.0).astype(BF16)

    def picked(side, start, width):
        factors = up[:, :, out_span(side, start, width)].reshape(held * ranks, width)
        return jnp.dot(pick, factors, preferred_element_type=F32).astype(BF16)

    def far_tokens(h):
        half = pl.ds(0, 2 * part_rows)
        remote(tok.at[half, :], far_tok.at[half, :], 2, z_sem.at[h], z_peer).wait_recv()

    def pick_part(dst, side, n):
        start, width = far_spans[n]
        dst[:, pl.ds(start, width)] = picked(side, start, width)

    pick_part(up_send, 1 - gx, 0)
    pick_part(up_send, 1 - gx, 1)
    relay(2)
    pick_part(up_send, 1 - gx, 2)
    remote(shrink_send, shrink_in, 3, shrink_sem, x_peer).wait_recv()
    shrink = (shrink_own[...] + shrink_in[0]) + (shrink_in[1] + shrink_in[2])
    low_send[...] = shrink.astype(BF16)
    low_copy = go(remote(low_send, low_in, 3, low_sem, x_peer))
    for n in range(early, len(x_copies)):
        go(x_copies[n])
    up_copy = go(remote(up_send, up_in, 1, up_sem, x_peer))
    relay(3)
    near_pair(4, hold=True)
    pick_part(up_peer, gx, 0)
    pick_part(up_peer, gx, 1)
    relay(4)
    pick_part(up_peer, gx, 2)
    near_step(1, 0)
    relay(5)
    near_step(1, 1)
    relay(6)
    near_step(1, 2)
    relay(7)

    def peer_part(n):
        start, width = far_spans[n]
        span = pl.ds(start, width)
        peer_extra[:, span] = expanded(low_in[...], up_peer[:, span])

    def local_part(n):
        start, width = far_spans[n]
        far_extra[:, pl.ds(start, width)] = expanded(
            low_send[...], up_own[:, out_span(1 - gx, start, width)]
        )

    far_tokens(0)
    far_dot(0, 0)
    relay(8)
    far_dot(0, 1)
    relay(9)
    far_dot(0, 2)
    far_pair(0, 0)
    low_copy.wait_recv()
    peer_part(0)
    far_pair(0, 1)
    relay(10)
    peer_part(1)
    far_pair(0, 2)
    peer_part(2)
    relay(11)

    far_tokens(1)
    far_dot(1, 0)
    relay(12)
    far_dot(1, 1)
    relay(13)
    far_dot(1, 2)
    far_pair(1, 0)
    relay(14)
    far_return(0, 0)
    far_pair(1, 1)
    relay(15)
    far_pair(1, 2)
    far_return(0, 1)

    far_tokens(2)
    far_dot(2, 0)
    far_dot(2, 1)
    far_return(0, 2)
    far_dot(2, 2)
    far_pair(2, 0)
    far_return(1, 0)
    far_pair(2, 1)
    far_pair(2, 2)

    far_tokens(3)
    far_dot(3, 0)
    far_return(1, 1)
    far_dot(3, 1)
    far_dot(3, 2)
    far_return(1, 2)
    far_pair(3, 0)
    far_pair(3, 1)
    far_return(2, 0)
    far_pair(3, 2)
    go(b_copies[near - 1])

    near_step(1, 3)
    far_return(2, 1)
    near_step(1, 4)
    local_part(0)
    far_return(2, 2)
    local_part(1)
    local_part(2)
    for n in range(far):
        finish_far(0, n)
    up_copy.wait_recv()
    far_return(3, 0)
    remote(a_send.at[1], a_in.at[1], 0, a_sem.at[near], core_peer).wait_recv()
    finish_near(0)
    finish_near(1)
    far_return(3, 1)
    finish_near(2)
    finish_near(3)
    far_return(3, 2)
    for h in range(1, STAGES - 1):
        for n in range(far):
            finish_far(h, n)
    finish_near(near - 1)
    for n in range(far):
        finish_far(STAGES - 1, n)

    d2d = w.at[pl.ds(0, 8 * block), :]
    remote(d2d, d2d, 0, name_sem, x_peer).wait_send()
    links = w.at[pl.ds(0, 3 * block + ranks), :]
    remote(links, links, 1, name_sem, x_peer).wait_send()
    remote(tok, tok, 2, name_sem, x_peer).wait_send()
    small = peer_extra.at[pl.ds(0, small_rows(ranks, block)), pl.ds(0, 128)]
    remote(small, small, 3, name_sem, x_peer).wait_send()


def small_rows(ranks, block):
    return (14 * ranks * block + 8 * 128 * 4) // (128 * 4)


def spans_of(cols, parts):
    unit = cols // sum(parts)
    return [(sum(parts[:n]) * unit, part * unit) for n, part in enumerate(parts)]


def fused_body(
    tokens,
    base_up_weight,
    adapter_down_weight,
    adapter_up_weight,
    block_adapter_index,
    request_rows,
):
    rows, depth = tokens.shape
    cols = base_up_weight.shape[1]
    blocks = block_adapter_index.shape[0]
    block = rows // blocks
    count, ranks, _ = adapter_down_weight.shape
    held, _, out_width = adapter_up_weight.shape
    near_spans = spans_of(cols, NEAR)
    far_spans = spans_of(cols, FAR)
    near, far = len(near_spans), len(far_spans)
    part_rows = block // STAGES
    in_hbm = pl.BlockSpec(memory_space=pltpu.HBM)

    dma = pltpu.SemaphoreType.DMA

    return pl.pallas_call(
        functools.partial(kernel, near_spans, far_spans),
        out_shape=pltpu.VMEM((block, out_width), BF16),
        in_specs=[in_hbm] * 6,
        out_specs=pl.BlockSpec(memory_space=pltpu.VMEM),
        scratch_shapes=[
            pltpu.SMEM((blocks,), jnp.int32),
            pltpu.SMEM((blocks,), jnp.int32),
            pltpu.VMEM((rows, depth), BF16),
            pltpu.VMEM((rows, depth), BF16),
            pltpu.VMEM((depth, cols), BF16),
            pltpu.VMEM((count, ranks, depth), BF16),
            pltpu.VMEM((held, ranks, out_width), BF16),
            pltpu.VMEM((8, 128), F32),
            pltpu.VMEM((8, 128), F32),
            pltpu.VMEM((ranks, out_width), BF16),
            pltpu.VMEM((ranks, cols), BF16),
            pltpu.VMEM((ranks, cols), BF16),
            pltpu.VMEM((ranks, cols), BF16),
            pltpu.VMEM((ranks, block), F32),
            pltpu.VMEM((3, ranks, block), F32),
            pltpu.VMEM((3, ranks, block), F32),
            pltpu.VMEM((ranks, block), BF16),
            pltpu.VMEM((ranks, block), BF16),
            pltpu.VMEM((block, cols), F32),
            pltpu.VMEM((block, cols), F32),
            pltpu.VMEM((2, block, cols), F32),
            pltpu.VMEM((2, block, cols), F32),
            pltpu.VMEM((2, block, cols), F32),
            pltpu.VMEM((STAGES, 2 * part_rows, cols), F32),
            pltpu.VMEM((STAGES, 2 * part_rows, cols), F32),
            pltpu.VMEM((STAGES, 2 * part_rows, cols), F32),
            pltpu.VMEM((block, cols), BF16),
            pltpu.VMEM((block, cols), BF16),
            pltpu.VMEM((STAGES, part_rows, cols), BF16),
            pltpu.VMEM((STAGES, part_rows, cols), BF16),
            pltpu.VMEM((STAGES, part_rows, cols), BF16),
            pltpu.VMEM((STAGES, part_rows, cols), BF16),
            dma((6,)),
            dma((near,)),
            dma((4,)),
            dma((near + 1,)),
            dma((2 * far,)),
            dma((near,)),
            dma((STAGES * far,)),
            dma((STAGES - 1 + far,)),
            dma((2 * CUTS * STAGES,)),
            dma((STAGES,)),
            dma,
            dma,
            dma,
            dma,
        ],
        compiler_params=pltpu.CompilerParams(
            collective_id=0, has_side_effects=True, vmem_limit_bytes=56 * 1024 * 1024
        ),
    )(
        block_adapter_index,
        request_rows,
        tokens,
        base_up_weight,
        adapter_down_weight,
        adapter_up_weight,
    )


def solution(mesh):
    in_specs = (
        P("gx", "gy"),
        P("gy", ("gz", "gx")),
        P(None, None, "gy"),
        P("gx", None, "gz"),
        P("gx"),
        P("gx"),
    )
    out_specs = P(("gx", "gy"), "gz")
    sizes = mesh.shape

    def body(*arrays):
        blocks = arrays[4].shape[0]
        paired = sizes["gx"] == 2 and sizes["gy"] == 4 and sizes["gz"] % 2 == 0
        cols = arrays[1].shape[1]
        cut = cols % (sum(NEAR) * 128) == 0
        cut = cut and arrays[0].shape[0] // blocks % (STAGES * 16) == 0
        if paired and cut and blocks == sizes["gy"]:
            return fused_body(*arrays)
        return general_body(*arrays)

    return jax.shard_map(body, mesh=mesh, in_specs=in_specs, out_specs=out_specs, check_vma=False)
```

```python
import functools

import jax
import jax.numpy as jnp
from jax import lax
from jax.experimental import pallas as pl
from jax.experimental.pallas import tpu as pltpu
from jax.sharding import PartitionSpec as P

F32 = jnp.float32
BF16 = jnp.bfloat16
STAGES = 4
CUTS = 2
NEAR = (2, 4, 4, 4, 4)
FAR = ((6, 8, 4),) * 4
PAIR = F32
MESH = pl.DeviceIdType.MESH


def general_body(
    tokens,
    base_up_weight,
    adapter_down_weight,
    adapter_up_weight,
    block_adapter_index,
    request_rows,
):
    rows, shard_width = tokens.shape
    groups = lax.axis_size("gy")
    blocks = block_adapter_index.shape[0]
    block = rows // blocks
    own_blocks = blocks // groups
    own_rows = own_blocks * block
    first = lax.axis_index("gy") * own_blocks
    count, rank_values, _ = adapter_down_weight.shape
    catalog = jnp.arange(count, dtype=jnp.int32)
    selected_adapters = (block_adapter_index[:, None] == catalog[None, :]).astype(BF16)
    chosen_down = jnp.dot(
        selected_adapters,
        adapter_down_weight.reshape(count, rank_values * shard_width),
        preferred_element_type=F32,
    )
    chosen_down = chosen_down.astype(BF16).reshape(blocks, rank_values, shard_width)
    tok_blocks = tokens.reshape(blocks, block, shard_width)
    shrink_part = jnp.einsum("bmd,brd->bmr", tok_blocks, chosen_down, preferred_element_type=F32)
    shrink_own = lax.psum_scatter(shrink_part, "gy", scatter_dimension=0, tiled=True)
    shrink_low = shrink_own.astype(BF16)
    adapter_factors = lax.all_gather(adapter_up_weight, "gx", axis=0, tiled=True)
    out_width = adapter_factors.shape[2]
    own_picks = lax.dynamic_slice_in_dim(selected_adapters, first, own_blocks, 0)
    chosen_up = jnp.dot(
        own_picks,
        adapter_factors.reshape(count, rank_values * out_width),
        preferred_element_type=F32,
    )
    chosen_up = chosen_up.astype(BF16).reshape(own_blocks, rank_values, out_width)
    expand = jnp.einsum("bmr,brf->bmf", shrink_low, chosen_up, preferred_element_type=F32)
    expand = expand.reshape(own_rows, out_width)
    partial_value = jnp.dot(
        tokens,
        lax.all_gather(base_up_weight, "gx", axis=1, tiled=True),
        preferred_element_type=F32,
    )
    extra = 2.0 * expand
    total = lax.psum_scatter(partial_value, "gy", scatter_dimension=0, tiled=True) + extra
    own_live = lax.dynamic_slice_in_dim(request_rows, first, own_blocks, 0)
    live_mask = (jnp.arange(block, dtype=jnp.int32)[None, :] < own_live[:, None]).reshape(
        own_rows, 1
    )
    return jnp.where(live_mask, total, 0.0).astype(BF16)


def kernel(
    near_spans,
    far_spans,
    index_hbm,
    live_hbm,
    tok_hbm,
    w_hbm,
    down_hbm,
    up_hbm,
    out_ref,
    index_ref,
    live_ref,
    tok,
    far_tok,
    w,
    down,
    up,
    name_send,
    name_in,
    up_own,
    up_send,
    up_in,
    up_peer,
    shrink_own,
    shrink_send,
    shrink_in,
    low_send,
    low_in,
    far_extra,
    peer_extra,
    a_send,
    a_in,
    keep,
    fa_send,
    fa_in,
    fkeep,
    b_send,
    b_in,
    fb_send,
    fb_in,
    c_send,
    c_in,
    send_sem,
    b_sem,
    c_sem,
    up_sem,
):
    gx = lax.axis_index("gx")
    gy = lax.axis_index("gy")
    gz = lax.axis_index("gz")
    core = lax.rem(gy, 2)
    yy = lax.div(gy, 2)
    y_far = 1 - yy
    zp = lax.rem(gz, 2)
    x_peer = {"gx": 1 - gx}
    core_peer = {"gy": gy + 1 - 2 * core}
    y_peer = {"gy": lax.rem(gy + 2, 4)}
    diagonal = {"gy": 3 - gy}
    z_peer = {"gz": gz + 1 - 2 * zp}
    block = out_ref.shape[0]
    cols = w.shape[1]
    held, ranks, _ = up.shape
    part_rows = block // STAGES
    piece = part_rows // CUTS
    near = len(near_spans)
    far = len(far_spans[0])

    def remote(src, dst, sent, sem, device):
        return pltpu.make_async_remote_copy(
            src_ref=src,
            dst_ref=dst,
            send_sem=send_sem.at[sent],
            recv_sem=sem,
            device_id=device,
            device_id_type=MESH,
        )

    def rows_at(block_at, first, count):
        return pl.ds(pl.multiple_of(block_at * block + first, count), count)

    def expanded(low, factor):
        return 2.0 * lax.dot_general(
            low, factor, (((0,), (0,)), ((), ())), preferred_element_type=F32
        )

    def live_rows(first, count):
        at = lax.broadcasted_iota(jnp.int32, (count, 1), 0) + first
        return at < live_ref[gy]

    def out_span(side, start, width):
        return pl.ds(pl.multiple_of(side * cols + start, 128), width)

    def finish_near(n):
        start, width = near_spans[n]
        span = pl.ds(start, width)
        remote(b_send.at[:, span], b_in.at[:, span], 1, b_sem.at[n], y_peer).wait_recv()
        total = keep[1, :, span] + b_in[:, span].astype(F32)
        out_ref[:, out_span(gx, start, width)] = jnp.where(
            live_rows(0, block), total, 0.0
        ).astype(BF16)

    def finish_far(h, n):
        start, width = far_spans[h][n]
        span = pl.ds(start, width)
        if h == STAGES - 1:
            remote(
                c_send.at[h, :, span],
                c_in.at[h, :, span],
                1,
                c_sem.at[h + n],
                x_peer,
            ).wait_recv()
        elif n == 0:
            remote(c_send.at[h], c_in.at[h], 1, c_sem.at[h], x_peer).wait_recv()
        rows = pl.ds(h * part_rows, part_rows)
        total = c_in[h, :, span].astype(F32) + far_extra[rows, span]
        out_ref[rows, out_span(1 - gx, start, width)] = jnp.where(
            live_rows(h * part_rows, part_rows), total, 0.0
        ).astype(BF16)

    def run(
        load_sem,
        w_sem,
        a_sem,
        fa_sem,
        fb_sem,
        x_sem,
        z_sem,
        shrink_sem,
        name_sem,
        low_sem,
    ):
        def load(src, dst, sem):
            copy = pltpu.make_async_copy(src, dst, sem)
            copy.start()
            return copy

        def tok_half(y_at, n):
            span = pl.ds(pl.multiple_of(y_at * 2 * block, 2 * block), 2 * block)
            return load(tok_hbm.at[span, :], tok.at[span, :], load_sem.at[n])

        def w_load(n):
            start, width = near_spans[n]
            span = pl.ds(start, width)
            return load(w_hbm.at[:, span], w.at[:, span], w_sem.at[n])

        tok_far_load = tok_half(y_far, 0)
        w_loads = [w_load(0)]
        tok_own_load = tok_half(yy, 1)
        index_load = load(index_hbm, index_ref, load_sem.at[2])
        live_load = load(live_hbm, live_ref, load_sem.at[3])
        w_loads += [w_load(n) for n in range(1, 3)]
        down_load = load(down_hbm, down, load_sem.at[4])
        w_loads += [w_load(n) for n in range(3, near)]

        barrier = pltpu.get_barrier_semaphore()
        for device in (x_peer, core_peer, y_peer, diagonal, z_peer):
            pl.semaphore_signal(barrier, inc=1, device_id=device, device_id_type=MESH)

        def go(copy):
            copy.start()
            return copy

        x_copies, z_copies = [], []
        for h in range(STAGES):
            for r in range(CUTS):
                for y_at in (y_far, yy):
                    span = rows_at(2 * y_at + zp, h * part_rows + r * piece, piece)
                    x_copies.append(
                        remote(
                            tok.at[span, :],
                            far_tok.at[span, :],
                            2,
                            x_sem.at[len(x_copies)],
                            x_peer,
                        )
                    )
                    z_copies.append(
                        remote(far_tok.at[span, :], far_tok.at[span, :], 2, z_sem.at[h], z_peer)
                    )

        def relay(n):
            x_copies[n].wait_recv()
            go(z_copies[n])

        a_copies, fa_copies, b_copies, fb_copies, c_copies = {}, {}, {}, {}, {}

        def near_dot(u, n):
            y_at = (y_far, yy)[u]
            start, width = near_spans[n]
            lhs = jnp.concatenate(
                [
                    tok[rows_at(2 * y_at + 1 - core, 0, block), :],
                    tok[rows_at(2 * y_at + core, 0, block), :],
                ],
                axis=0,
            )
            span = slice(start, start + width)
            part = jnp.dot(lhs, w[:, span], preferred_element_type=F32)
            a_send[u, :, span] = part[:block].astype(a_send.dtype)
            keep[u, :, span] = part[block:]

        def near_give(u, n):
            start, width = near_spans[n]
            span = pl.ds(start, width)
            a_copies[u, n] = go(
                remote(
                    a_send.at[u, :, span],
                    a_in.at[u, :, span],
                    0,
                    a_sem.at[near if u else n],
                    core_peer,
                )
            )

        def near_pair(n, hold=False):
            start, width = near_spans[n]
            span = pl.ds(start, width)
            a_copies[0, n].wait_recv()
            b_send[:, span] = (keep[0, :, span] + a_in[0, :, span].astype(F32)).astype(BF16)
            b_copies[n] = remote(b_send.at[:, span], b_in.at[:, span], 1, b_sem.at[n], y_peer)
            if not hold:
                go(b_copies[n])

        def far_dot(h, n):
            start, width = far_spans[h][n]
            lhs = jnp.concatenate(
                [
                    far_tok[rows_at(2 * y_at + c, h * part_rows, part_rows), :]
                    for c in (1 - core, core)
                    for y_at in (y_far, yy)
                ],
                axis=0,
            )
            span = slice(start, start + width)
            part = jnp.dot(lhs, w[:, span], preferred_element_type=F32)
            fa_send[h, :, span] = part[: 2 * part_rows].astype(fa_send.dtype)
            fkeep[h, :, span] = part[2 * part_rows :]
            span = pl.ds(start, width)
            fa_copies[h, n] = go(
                remote(
                    fa_send.at[h, :, span],
                    fa_in.at[h, :, span],
                    0,
                    fa_sem.at[h % 2 * far + n],
                    core_peer,
                )
            )

        def far_pair(h, n):
            start, width = far_spans[h][n]
            span = pl.ds(start, width)
            fa_copies[h, n].wait_recv()
            out_rows = pl.ds(0, part_rows)
            fb_send[h, :, span] = (
                fkeep[h, out_rows, span] + fa_in[h, out_rows, span].astype(F32)
            ).astype(BF16)
            fb_copies[h, n] = go(
                remote(
                    fb_send.at[h, :, span],
                    fb_in.at[h, :, span],
                    1,
                    fb_sem.at[h * far + n],
                    y_peer,
                )
            )

        def far_return(h, n):
            start, width = far_spans[h][n]
            span = pl.ds(start, width)
            own_rows = pl.ds(part_rows, part_rows)
            fb_copies[h, n].wait_recv()
            total = fkeep[h, own_rows, span] + fa_in[h, own_rows, span].astype(F32)
            total += fb_in[h, :, span].astype(F32)
            total += peer_extra[pl.ds(h * part_rows, part_rows), span]
            c_send[h, :, span] = total.astype(BF16)
            c_copies[h, n] = go(
                remote(
                    c_send.at[h, :, span],
                    c_in.at[h, :, span],
                    1,
                    c_sem.at[h + n if h == STAGES - 1 else h],
                    x_peer,
                )
            )

        def ready_near(n):
            start, width = near_spans[n]
            span = pl.ds(start, width)
            factor = up_own[:, out_span(gx, start, width)] + up_in[:, span]
            keep[1, :, span] += a_in[1, :, span].astype(F32) + expanded(low_send[...], factor)

        def near_step(u, n):
            if u == 0:
                w_loads[n].wait()
            near_dot(u, n)
            near_give(u, n)

        tok_far_load.wait()
        w_loads[0].wait()
        near_dot(0, 0)
        tok_own_load.wait()
        pl.semaphore_wait(barrier, 5)
        early = len(x_copies) // 2
        for n in range(2):
            go(x_copies[n])
        index_load.wait()
        live_load.wait()
        name_send[...] = jnp.full(name_send.shape, index_ref[gy].astype(F32))
        name_copy = go(remote(name_send, name_in, 3, name_sem, x_peer))
        for n in range(2, early):
            go(x_copies[n])
        near_give(0, 0)

        shrink_copies = []

        def shrink_part(at):
            return lax.dot_general(
                down[index_ref[at]],
                tok[rows_at(at, 0, block), :],
                (((1,), (1,)), ((), ())),
                preferred_element_type=F32,
            )

        def shrink_give(d, device):
            shrink_send[d] = shrink_part(device["gy"])
            shrink_copies.append(
                go(remote(shrink_send.at[d], shrink_in.at[d], 3, shrink_sem, device))
            )

        near_step(0, 1)
        up_load = load(up_hbm, up, load_sem.at[5])
        near_step(0, 2)
        near_pair(0)
        down_load.wait()
        shrink_give(0, y_peer)
        shrink_give(1, diagonal)
        near_pair(1)
        near_step(0, 3)
        shrink_give(2, core_peer)
        near_pair(2)
        near_step(0, 4)
        relay(0)
        shrink_own[...] = shrink_part(gy)
        near_pair(3)
        relay(1)

        up_load.wait()
        slot = index_ref[gy] - gx * held
        mine = up[jnp.clip(slot, 0, held - 1)]
        here = jnp.logical_and(slot >= 0, slot < held)
        up_own[...] = jnp.where(here, mine, jnp.zeros_like(mine))
        name_copy.wait_recv()
        rank_at = lax.broadcasted_iota(jnp.int32, (ranks, held * ranks), 0)
        slot_at = lax.broadcasted_iota(jnp.int32, (ranks, held * ranks), 1) + gx * held * ranks
        wanted = name_in[0:1, 0:1] * float(ranks)
        hit = (slot_at - rank_at).astype(F32) == wanted
        pick = jnp.where(hit, 1.0, 0.0).astype(BF16)

        def picked(side, start, width):
            factors = up[:, :, out_span(side, start, width)].reshape(held * ranks, width)
            return jnp.dot(pick, factors, preferred_element_type=F32).astype(BF16)

        def far_tokens(h):
            half = pl.ds(0, 2 * part_rows)
            remote(tok.at[half, :], far_tok.at[half, :], 2, z_sem.at[h], z_peer).wait_recv()

        def pick_part(dst, side, n):
            start, width = far_spans[1][n]
            dst[:, pl.ds(start, width)] = picked(side, start, width)

        pick_part(up_send, 1 - gx, 0)
        pick_part(up_send, 1 - gx, 1)
        relay(2)
        pick_part(up_send, 1 - gx, 2)
        remote(shrink_send, shrink_in, 3, shrink_sem, x_peer).wait_recv()
        shrink = (shrink_own[...] + shrink_in[0]) + (shrink_in[1] + shrink_in[2])
        low_send[...] = shrink.astype(BF16)
        low_copy = go(remote(low_send, low_in, 3, low_sem, x_peer))
        for n in range(early, len(x_copies)):
            go(x_copies[n])
        up_copy = go(remote(up_send, up_in, 1, up_sem, x_peer))
        relay(3)
        near_pair(4, hold=True)
        pick_part(up_peer, gx, 0)
        pick_part(up_peer, gx, 1)
        relay(4)
        pick_part(up_peer, gx, 2)
        near_step(1, 0)
        relay(5)
        near_step(1, 1)
        relay(6)
        near_step(1, 2)
        relay(7)

        def peer_part(n):
            start, width = far_spans[1][n]
            span = pl.ds(start, width)
            peer_extra[:, span] = expanded(low_in[...], up_peer[:, span])

        def local_part(n):
            start, width = far_spans[1][n]
            far_extra[:, pl.ds(start, width)] = expanded(
                low_send[...], up_own[:, out_span(1 - gx, start, width)]
            )

        far_tokens(0)
        far_dot(0, 0)
        relay(8)
        far_dot(0, 1)
        relay(9)
        far_dot(0, 2)
        far_pair(0, 0)
        low_copy.wait_recv()
        peer_part(0)
        far_pair(0, 1)
        relay(10)
        peer_part(1)
        far_pair(0, 2)
        peer_part(2)
        relay(11)

        far_tokens(1)
        far_dot(1, 0)
        relay(12)
        far_dot(1, 1)
        relay(13)
        far_dot(1, 2)
        far_pair(1, 0)
        relay(14)
        far_return(0, 0)
        far_pair(1, 1)
        relay(15)
        far_pair(1, 2)
        far_return(0, 1)

        far_tokens(2)
        far_dot(2, 0)
        far_dot(2, 1)
        far_return(0, 2)
        far_dot(2, 2)
        far_pair(2, 0)
        far_return(1, 0)
        far_pair(2, 1)
        far_pair(2, 2)

        far_tokens(3)
        far_dot(3, 0)
        far_return(1, 1)
        far_dot(3, 1)
        far_dot(3, 2)
        far_return(1, 2)
        far_pair(3, 0)
        far_pair(3, 1)
        far_return(2, 0)
        far_pair(3, 2)
        go(b_copies[near - 1])

        near_step(1, 3)
        far_return(2, 1)
        near_step(1, 4)
        local_part(0)
        far_return(2, 2)
        local_part(1)
        local_part(2)
        for n in range(far):
            finish_far(0, n)
        up_copy.wait_recv()
        far_return(3, 0)
        remote(a_send.at[1], a_in.at[1], 0, a_sem.at[near], core_peer).wait_recv()
        ready_near(0)
        ready_near(1)
        ready_near(2)
        far_return(3, 1)
        ready_near(3)
        far_return(3, 2)
        ready_near(4)

    dma = pltpu.SemaphoreType.DMA
    pl.run_scoped(
        run,
        dma((6,)),
        dma((near,)),
        dma((near + 1,)),
        dma((2 * far,)),
        dma((STAGES * far,)),
        dma((2 * CUTS * STAGES,)),
        dma((STAGES,)),
        dma,
        dma,
        dma,
    )
    for n in range(near - 1):
        finish_near(n)
    for h in range(1, STAGES - 1):
        for n in range(far):
            finish_far(h, n)
    for n in range(far - 1):
        finish_far(STAGES - 1, n)
    finish_near(near - 1)
    finish_far(STAGES - 1, far - 1)

    d2d = w.at[pl.ds(0, 2 * jnp.dtype(PAIR).itemsize * block), :]
    remote(d2d, d2d, 0, up_sem, x_peer).wait_send()
    links = w.at[pl.ds(0, 3 * block + ranks), :]
    remote(links, links, 1, up_sem, x_peer).wait_send()
    remote(tok, tok, 2, up_sem, x_peer).wait_send()
    small = peer_extra.at[pl.ds(0, small_rows(ranks, block)), pl.ds(0, 128)]
    remote(small, small, 3, up_sem, x_peer).wait_send()


def small_rows(ranks, block):
    return (14 * ranks * block + 8 * 128 * 4) // (128 * 4)


def spans_of(cols, parts):
    unit = cols // sum(parts)
    return [(sum(parts[:n]) * unit, part * unit) for n, part in enumerate(parts)]


def fused_body(
    tokens,
    base_up_weight,
    adapter_down_weight,
    adapter_up_weight,
    block_adapter_index,
    request_rows,
):
    rows, depth = tokens.shape
    cols = base_up_weight.shape[1]
    blocks = block_adapter_index.shape[0]
    block = rows // blocks
    count, ranks, _ = adapter_down_weight.shape
    held, _, out_width = adapter_up_weight.shape
    near_spans = spans_of(cols, NEAR)
    far_spans = [spans_of(cols, parts) for parts in FAR]
    near, far = len(near_spans), len(far_spans[0])
    part_rows = block // STAGES
    in_hbm = pl.BlockSpec(memory_space=pltpu.HBM)

    dma = pltpu.SemaphoreType.DMA

    return pl.pallas_call(
        functools.partial(kernel, near_spans, far_spans),
        out_shape=pltpu.VMEM((block, out_width), BF16),
        in_specs=[in_hbm] * 6,
        out_specs=pl.BlockSpec(memory_space=pltpu.VMEM),
        scratch_shapes=[
            pltpu.SMEM((blocks,), jnp.int32),
            pltpu.SMEM((blocks,), jnp.int32),
            pltpu.VMEM((rows, depth), BF16),
            pltpu.VMEM((rows, depth), BF16),
            pltpu.VMEM((depth, cols), BF16),
            pltpu.VMEM((count, ranks, depth), BF16),
            pltpu.VMEM((held, ranks, out_width), BF16),
            pltpu.VMEM((8, 128), F32),
            pltpu.VMEM((8, 128), F32),
            pltpu.VMEM((ranks, out_width), BF16),
            pltpu.VMEM((ranks, cols), BF16),
            pltpu.VMEM((ranks, cols), BF16),
            pltpu.VMEM((ranks, cols), BF16),
            pltpu.VMEM((ranks, block), F32),
            pltpu.VMEM((3, ranks, block), F32),
            pltpu.VMEM((3, ranks, block), F32),
            pltpu.VMEM((ranks, block), BF16),
            pltpu.VMEM((ranks, block), BF16),
            pltpu.VMEM((block, cols), F32),
            pltpu.VMEM((block, cols), F32),
            pltpu.VMEM((2, block, cols), PAIR),
            pltpu.VMEM((2, block, cols), PAIR),
            pltpu.VMEM((2, block, cols), F32),
            pltpu.VMEM((STAGES, 2 * part_rows, cols), PAIR),
            pltpu.VMEM((STAGES, 2 * part_rows, cols), PAIR),
            pltpu.VMEM((STAGES, 2 * part_rows, cols), F32),
            pltpu.VMEM((block, cols), BF16),
            pltpu.VMEM((block, cols), BF16),
            pltpu.VMEM((STAGES, part_rows, cols), BF16),
            pltpu.VMEM((STAGES, part_rows, cols), BF16),
            pltpu.VMEM((STAGES, part_rows, cols), BF16),
            pltpu.VMEM((STAGES, part_rows, cols), BF16),
            dma((4,)),
            dma((near,)),
            dma((STAGES - 1 + far,)),
            dma,
        ],
        compiler_params=pltpu.CompilerParams(
            collective_id=0, has_side_effects=True, vmem_limit_bytes=56 * 1024 * 1024
        ),
    )(
        block_adapter_index,
        request_rows,
        tokens,
        base_up_weight,
        adapter_down_weight,
        adapter_up_weight,
    )


def solution(mesh):
    in_specs = (
        P("gx", "gy"),
        P("gy", ("gz", "gx")),
        P(None, None, "gy"),
        P("gx", None, "gz"),
        P("gx"),
        P("gx"),
    )
    out_specs = P(("gx", "gy"), "gz")
    sizes = mesh.shape

    def body(*arrays):
        blocks = arrays[4].shape[0]
        paired = sizes["gx"] == 2 and sizes["gy"] == 4 and sizes["gz"] % 2 == 0
        cols = arrays[1].shape[1]
        cut = cols % (sum(NEAR) * 128) == 0
        cut = cut and arrays[0].shape[0] // blocks % (STAGES * 16) == 0
        if paired and cut and blocks == sizes["gy"]:
            return fused_body(*arrays)
        return general_body(*arrays)

    return jax.shard_map(body, mesh=mesh, in_specs=in_specs, out_specs=out_specs, check_vma=False)
```

```python
import functools

import jax
import jax.numpy as jnp
from jax import lax
from jax.experimental import pallas as pl
from jax.experimental.pallas import tpu as pltpu
from jax.sharding import PartitionSpec as P

F32 = jnp.float32
BF16 = jnp.bfloat16
STAGES = 4
CUTS = 2
NEAR = (2, 4, 4, 4, 4)
FAR = ((6, 8, 4),) * 4
PAIR = F32
MESH = pl.DeviceIdType.MESH


def general_body(
    tokens,
    base_up_weight,
    adapter_down_weight,
    adapter_up_weight,
    block_adapter_index,
    request_rows,
):
    rows, shard_width = tokens.shape
    groups = lax.axis_size("gy")
    blocks = block_adapter_index.shape[0]
    block = rows // blocks
    own_blocks = blocks // groups
    own_rows = own_blocks * block
    first = lax.axis_index("gy") * own_blocks
    count, rank_values, _ = adapter_down_weight.shape
    catalog = jnp.arange(count, dtype=jnp.int32)
    selected_adapters = (block_adapter_index[:, None] == catalog[None, :]).astype(BF16)
    chosen_down = jnp.dot(
        selected_adapters,
        adapter_down_weight.reshape(count, rank_values * shard_width),
        preferred_element_type=F32,
    )
    chosen_down = chosen_down.astype(BF16).reshape(blocks, rank_values, shard_width)
    tok_blocks = tokens.reshape(blocks, block, shard_width)
    shrink_part = jnp.einsum("bmd,brd->bmr", tok_blocks, chosen_down, preferred_element_type=F32)
    shrink_own = lax.psum_scatter(shrink_part, "gy", scatter_dimension=0, tiled=True)
    shrink_low = shrink_own.astype(BF16)
    adapter_factors = lax.all_gather(adapter_up_weight, "gx", axis=0, tiled=True)
    out_width = adapter_factors.shape[2]
    own_picks = lax.dynamic_slice_in_dim(selected_adapters, first, own_blocks, 0)
    chosen_up = jnp.dot(
        own_picks,
        adapter_factors.reshape(count, rank_values * out_width),
        preferred_element_type=F32,
    )
    chosen_up = chosen_up.astype(BF16).reshape(own_blocks, rank_values, out_width)
    expand = jnp.einsum("bmr,brf->bmf", shrink_low, chosen_up, preferred_element_type=F32)
    expand = expand.reshape(own_rows, out_width)
    partial_value = jnp.dot(
        tokens,
        lax.all_gather(base_up_weight, "gx", axis=1, tiled=True),
        preferred_element_type=F32,
    )
    extra = 2.0 * expand
    total = lax.psum_scatter(partial_value, "gy", scatter_dimension=0, tiled=True) + extra
    own_live = lax.dynamic_slice_in_dim(request_rows, first, own_blocks, 0)
    live_mask = (jnp.arange(block, dtype=jnp.int32)[None, :] < own_live[:, None]).reshape(
        own_rows, 1
    )
    return jnp.where(live_mask, total, 0.0).astype(BF16)


def kernel(
    near_spans,
    far_spans,
    index_hbm,
    live_hbm,
    tok_hbm,
    w_hbm,
    down_hbm,
    up_hbm,
    out_ref,
    index_ref,
    live_ref,
    tok,
    far_tok,
    w,
    down,
    up,
    name_send,
    name_in,
    up_own,
    up_send,
    up_in,
    up_peer,
    shrink_own,
    shrink_send,
    shrink_in,
    low_send,
    low_in,
    far_extra,
    peer_extra,
    a_send,
    a_in,
    keep,
    fa_send,
    fa_in,
    fkeep,
    b_send,
    b_in,
    fb_send,
    fb_in,
    c_send,
    c_in,
    send_sem,
    b_last,
    c_last,
):
    gx = lax.axis_index("gx")
    gy = lax.axis_index("gy")
    gz = lax.axis_index("gz")
    core = lax.rem(gy, 2)
    yy = lax.div(gy, 2)
    y_far = 1 - yy
    zp = lax.rem(gz, 2)
    x_peer = {"gx": 1 - gx}
    core_peer = {"gy": gy + 1 - 2 * core}
    y_peer = {"gy": lax.rem(gy + 2, 4)}
    diagonal = {"gy": 3 - gy}
    z_peer = {"gz": gz + 1 - 2 * zp}
    block = out_ref.shape[0]
    cols = w.shape[1]
    held, ranks, _ = up.shape
    part_rows = block // STAGES
    piece = part_rows // CUTS
    near = len(near_spans)
    far = len(far_spans[0])

    def remote(src, dst, sent, sem, device):
        return pltpu.make_async_remote_copy(
            src_ref=src,
            dst_ref=dst,
            send_sem=send_sem.at[sent],
            recv_sem=sem,
            device_id=device,
            device_id_type=MESH,
        )

    def rows_at(block_at, first, count):
        return pl.ds(pl.multiple_of(block_at * block + first, count), count)

    def expanded(low, factor):
        return 2.0 * lax.dot_general(
            low, factor, (((0,), (0,)), ((), ())), preferred_element_type=F32
        )

    def live_rows(first, count):
        at = lax.broadcasted_iota(jnp.int32, (count, 1), 0) + first
        return at < live_ref[gy]

    def out_span(side, start, width):
        return pl.ds(pl.multiple_of(side * cols + start, 128), width)

    def finish_near(n, sem):
        start, width = near_spans[n]
        span = pl.ds(start, width)
        remote(b_send.at[:, span], b_in.at[:, span], 1, sem, y_peer).wait_recv()
        total = keep[1, :, span] + b_in[:, span].astype(F32)
        out_ref[:, out_span(gx, start, width)] = jnp.where(
            live_rows(0, block), total, 0.0
        ).astype(BF16)

    def finish_far(h, n, sem):
        start, width = far_spans[h][n]
        span = pl.ds(start, width)
        if h == STAGES - 1:
            remote(
                c_send.at[h, :, span],
                c_in.at[h, :, span],
                1,
                sem,
                x_peer,
            ).wait_recv()
        elif n == 0:
            remote(c_send.at[h], c_in.at[h], 1, sem, x_peer).wait_recv()
        rows = pl.ds(h * part_rows, part_rows)
        total = c_in[h, :, span].astype(F32) + far_extra[rows, span]
        out_ref[rows, out_span(1 - gx, start, width)] = jnp.where(
            live_rows(h * part_rows, part_rows), total, 0.0
        ).astype(BF16)

    def run(
        load_sem,
        w_sem,
        a_sem,
        fa_sem,
        fb_sem,
        x_sem,
        z_sem,
        shrink_sem,
        name_sem,
        low_sem,
        b_sem,
        c_sem,
        up_sem,
    ):
        def load(src, dst, sem):
            copy = pltpu.make_async_copy(src, dst, sem)
            copy.start()
            return copy

        def tok_half(y_at, n):
            span = pl.ds(pl.multiple_of(y_at * 2 * block, 2 * block), 2 * block)
            return load(tok_hbm.at[span, :], tok.at[span, :], load_sem.at[n])

        def w_load(n):
            start, width = near_spans[n]
            span = pl.ds(start, width)
            return load(w_hbm.at[:, span], w.at[:, span], w_sem.at[n])

        tok_far_load = tok_half(y_far, 0)
        w_loads = [w_load(0)]
        tok_own_load = tok_half(yy, 1)
        index_load = load(index_hbm, index_ref, load_sem.at[2])
        live_load = load(live_hbm, live_ref, load_sem.at[3])
        w_loads += [w_load(n) for n in range(1, 3)]
        down_load = load(down_hbm, down, load_sem.at[4])
        w_loads += [w_load(n) for n in range(3, near)]

        barrier = pltpu.get_barrier_semaphore()
        for device in (x_peer, core_peer, y_peer, diagonal, z_peer):
            pl.semaphore_signal(barrier, inc=1, device_id=device, device_id_type=MESH)

        def go(copy):
            copy.start()
            return copy

        x_copies, z_copies = [], []
        for h in range(STAGES):
            for r in range(CUTS):
                for y_at in (y_far, yy):
                    span = rows_at(2 * y_at + zp, h * part_rows + r * piece, piece)
                    x_copies.append(
                        remote(
                            tok.at[span, :],
                            far_tok.at[span, :],
                            2,
                            x_sem.at[len(x_copies)],
                            x_peer,
                        )
                    )
                    z_copies.append(
                        remote(far_tok.at[span, :], far_tok.at[span, :], 2, z_sem.at[h], z_peer)
                    )

        def relay(n):
            x_copies[n].wait_recv()
            go(z_copies[n])

        a_copies, fa_copies, b_copies, fb_copies, c_copies = {}, {}, {}, {}, {}

        def near_dot(u, n):
            y_at = (y_far, yy)[u]
            start, width = near_spans[n]
            lhs = jnp.concatenate(
                [
                    tok[rows_at(2 * y_at + 1 - core, 0, block), :],
                    tok[rows_at(2 * y_at + core, 0, block), :],
                ],
                axis=0,
            )
            span = slice(start, start + width)
            part = jnp.dot(lhs, w[:, span], preferred_element_type=F32)
            a_send[u, :, span] = part[:block].astype(a_send.dtype)
            keep[u, :, span] = part[block:]

        def near_give(u, n):
            start, width = near_spans[n]
            span = pl.ds(start, width)
            a_copies[u, n] = go(
                remote(
                    a_send.at[u, :, span],
                    a_in.at[u, :, span],
                    0,
                    a_sem.at[near if u else n],
                    core_peer,
                )
            )

        def near_pair(n, hold=False):
            start, width = near_spans[n]
            span = pl.ds(start, width)
            a_copies[0, n].wait_recv()
            b_send[:, span] = (keep[0, :, span] + a_in[0, :, span].astype(F32)).astype(BF16)
            b_copies[n] = remote(b_send.at[:, span], b_in.at[:, span], 1, b_last if n == near - 1 else b_sem.at[n], y_peer)
            if not hold:
                go(b_copies[n])

        def far_dot(h, n):
            start, width = far_spans[h][n]
            lhs = jnp.concatenate(
                [
                    far_tok[rows_at(2 * y_at + c, h * part_rows, part_rows), :]
                    for c in (1 - core, core)
                    for y_at in (y_far, yy)
                ],
                axis=0,
            )
            span = slice(start, start + width)
            part = jnp.dot(lhs, w[:, span], preferred_element_type=F32)
            fa_send[h, :, span] = part[: 2 * part_rows].astype(fa_send.dtype)
            fkeep[h, :, span] = part[2 * part_rows :]
            span = pl.ds(start, width)
            fa_copies[h, n] = go(
                remote(
                    fa_send.at[h, :, span],
                    fa_in.at[h, :, span],
                    0,
                    fa_sem.at[h % 2 * far + n],
                    core_peer,
                )
            )

        def far_pair(h, n):
            start, width = far_spans[h][n]
            span = pl.ds(start, width)
            fa_copies[h, n].wait_recv()
            out_rows = pl.ds(0, part_rows)
            fb_send[h, :, span] = (
                fkeep[h, out_rows, span] + fa_in[h, out_rows, span].astype(F32)
            ).astype(BF16)
            fb_copies[h, n] = go(
                remote(
                    fb_send.at[h, :, span],
                    fb_in.at[h, :, span],
                    1,
                    fb_sem.at[h * far + n],
                    y_peer,
                )
            )

        def far_return(h, n):
            start, width = far_spans[h][n]
            span = pl.ds(start, width)
            own_rows = pl.ds(part_rows, part_rows)
            fb_copies[h, n].wait_recv()
            total = fkeep[h, own_rows, span] + fa_in[h, own_rows, span].astype(F32)
            total += fb_in[h, :, span].astype(F32)
            total += peer_extra[pl.ds(h * part_rows, part_rows), span]
            c_send[h, :, span] = total.astype(BF16)
            c_copies[h, n] = go(
                remote(
                    c_send.at[h, :, span],
                    c_in.at[h, :, span],
                    1,
                    c_last.at[n] if h == STAGES - 1 else c_sem.at[h],
                    x_peer,
                )
            )

        def ready_near(n):
            start, width = near_spans[n]
            span = pl.ds(start, width)
            factor = up_own[:, out_span(gx, start, width)] + up_in[:, span]
            keep[1, :, span] += a_in[1, :, span].astype(F32) + expanded(low_send[...], factor)

        def near_step(u, n):
            if u == 0:
                w_loads[n].wait()
            near_dot(u, n)
            near_give(u, n)

        tok_far_load.wait()
        w_loads[0].wait()
        near_dot(0, 0)
        tok_own_load.wait()
        pl.semaphore_wait(barrier, 5)
        early = len(x_copies) // 2
        for n in range(2):
            go(x_copies[n])
        index_load.wait()
        live_load.wait()
        name_send[...] = jnp.full(name_send.shape, index_ref[gy].astype(F32))
        name_copy = go(remote(name_send, name_in, 3, name_sem, x_peer))
        for n in range(2, early):
            go(x_copies[n])
        near_give(0, 0)

        shrink_copies = []

        def shrink_part(at):
            return lax.dot_general(
                down[index_ref[at]],
                tok[rows_at(at, 0, block), :],
                (((1,), (1,)), ((), ())),
                preferred_element_type=F32,
            )

        def shrink_give(d, device):
            shrink_send[d] = shrink_part(device["gy"])
            shrink_copies.append(
                go(remote(shrink_send.at[d], shrink_in.at[d], 3, shrink_sem, device))
            )

        near_step(0, 1)
        up_load = load(up_hbm, up, load_sem.at[5])
        near_step(0, 2)
        near_pair(0)
        down_load.wait()
        shrink_give(0, y_peer)
        shrink_give(1, diagonal)
        near_pair(1)
        near_step(0, 3)
        shrink_give(2, core_peer)
        near_pair(2)
        near_step(0, 4)
        relay(0)
        shrink_own[...] = shrink_part(gy)
        near_pair(3)
        relay(1)

        up_load.wait()
        slot = index_ref[gy] - gx * held
        mine = up[jnp.clip(slot, 0, held - 1)]
        here = jnp.logical_and(slot >= 0, slot < held)
        up_own[...] = jnp.where(here, mine, jnp.zeros_like(mine))
        name_copy.wait_recv()
        rank_at = lax.broadcasted_iota(jnp.int32, (ranks, held * ranks), 0)
        slot_at = lax.broadcasted_iota(jnp.int32, (ranks, held * ranks), 1) + gx * held * ranks
        wanted = name_in[0:1, 0:1] * float(ranks)
        hit = (slot_at - rank_at).astype(F32) == wanted
        pick = jnp.where(hit, 1.0, 0.0).astype(BF16)

        def picked(side, start, width):
            factors = up[:, :, out_span(side, start, width)].reshape(held * ranks, width)
            return jnp.dot(pick, factors, preferred_element_type=F32).astype(BF16)

        def far_tokens(h):
            half = pl.ds(0, 2 * part_rows)
            remote(tok.at[half, :], far_tok.at[half, :], 2, z_sem.at[h], z_peer).wait_recv()

        def pick_part(dst, side, n):
            start, width = far_spans[1][n]
            dst[:, pl.ds(start, width)] = picked(side, start, width)

        pick_part(up_send, 1 - gx, 0)
        pick_part(up_send, 1 - gx, 1)
        relay(2)
        pick_part(up_send, 1 - gx, 2)
        remote(shrink_send, shrink_in, 3, shrink_sem, x_peer).wait_recv()
        shrink = (shrink_own[...] + shrink_in[0]) + (shrink_in[1] + shrink_in[2])
        low_send[...] = shrink.astype(BF16)
        low_copy = go(remote(low_send, low_in, 3, low_sem, x_peer))
        for n in range(early, len(x_copies)):
            go(x_copies[n])
        up_copy = go(remote(up_send, up_in, 1, up_sem, x_peer))
        relay(3)
        near_pair(4, hold=True)
        pick_part(up_peer, gx, 0)
        pick_part(up_peer, gx, 1)
        relay(4)
        pick_part(up_peer, gx, 2)
        near_step(1, 0)
        relay(5)
        near_step(1, 1)
        relay(6)
        near_step(1, 2)
        relay(7)

        def peer_part(n):
            start, width = far_spans[1][n]
            span = pl.ds(start, width)
            peer_extra[:, span] = expanded(low_in[...], up_peer[:, span])

        def local_part(n):
            start, width = far_spans[1][n]
            far_extra[:, pl.ds(start, width)] = expanded(
                low_send[...], up_own[:, out_span(1 - gx, start, width)]
            )

        far_tokens(0)
        far_dot(0, 0)
        relay(8)
        far_dot(0, 1)
        relay(9)
        far_dot(0, 2)
        far_pair(0, 0)
        low_copy.wait_recv()
        peer_part(0)
        far_pair(0, 1)
        relay(10)
        peer_part(1)
        far_pair(0, 2)
        peer_part(2)
        relay(11)

        far_tokens(1)
        far_dot(1, 0)
        relay(12)
        far_dot(1, 1)
        relay(13)
        far_dot(1, 2)
        far_pair(1, 0)
        relay(14)
        far_return(0, 0)
        far_pair(1, 1)
        relay(15)
        far_pair(1, 2)
        far_return(0, 1)

        far_tokens(2)
        far_dot(2, 0)
        far_dot(2, 1)
        far_return(0, 2)
        far_dot(2, 2)
        far_pair(2, 0)
        far_return(1, 0)
        far_pair(2, 1)
        far_pair(2, 2)

        far_tokens(3)
        far_dot(3, 0)
        far_return(1, 1)
        far_dot(3, 1)
        far_dot(3, 2)
        far_return(1, 2)
        far_pair(3, 0)
        far_pair(3, 1)
        far_return(2, 0)
        far_pair(3, 2)
        go(b_copies[near - 1])

        near_step(1, 3)
        far_return(2, 1)
        near_step(1, 4)
        local_part(0)
        far_return(2, 2)
        local_part(1)
        local_part(2)
        for n in range(far):
            finish_far(0, n, c_sem.at[0])
        up_copy.wait_recv()
        far_return(3, 0)
        remote(a_send.at[1], a_in.at[1], 0, a_sem.at[near], core_peer).wait_recv()
        ready_near(0)
        ready_near(1)
        ready_near(2)
        far_return(3, 1)
        ready_near(3)
        far_return(3, 2)
        ready_near(4)
        for n in range(near - 1):
            finish_near(n, b_sem.at[n])
        for h in range(1, STAGES - 1):
            for n in range(far):
                finish_far(h, n, c_sem.at[h])

    dma = pltpu.SemaphoreType.DMA
    pl.run_scoped(
        run,
        dma((6,)),
        dma((near,)),
        dma((near + 1,)),
        dma((2 * far,)),
        dma((STAGES * far,)),
        dma((2 * CUTS * STAGES,)),
        dma((STAGES,)),
        dma,
        dma,
        dma,
        dma((near - 1,)),
        dma((STAGES - 1,)),
        dma,
    )
    for n in range(far - 1):
        finish_far(STAGES - 1, n, c_last.at[n])
    finish_near(near - 1, b_last)
    finish_far(STAGES - 1, far - 1, c_last.at[far - 1])

    d2d = w.at[pl.ds(0, 2 * jnp.dtype(PAIR).itemsize * block), :]
    remote(d2d, d2d, 0, b_last, x_peer).wait_send()
    links = w.at[pl.ds(0, 3 * block + ranks), :]
    remote(links, links, 1, b_last, x_peer).wait_send()
    remote(tok, tok, 2, b_last, x_peer).wait_send()
    small = peer_extra.at[pl.ds(0, small_rows(ranks, block)), pl.ds(0, 128)]
    remote(small, small, 3, b_last, x_peer).wait_send()


def small_rows(ranks, block):
    return (14 * ranks * block + 8 * 128 * 4) // (128 * 4)


def spans_of(cols, parts):
    unit = cols // sum(parts)
    return [(sum(parts[:n]) * unit, part * unit) for n, part in enumerate(parts)]


def fused_body(
    tokens,
    base_up_weight,
    adapter_down_weight,
    adapter_up_weight,
    block_adapter_index,
    request_rows,
):
    rows, depth = tokens.shape
    cols = base_up_weight.shape[1]
    blocks = block_adapter_index.shape[0]
    block = rows // blocks
    count, ranks, _ = adapter_down_weight.shape
    held, _, out_width = adapter_up_weight.shape
    near_spans = spans_of(cols, NEAR)
    far_spans = [spans_of(cols, parts) for parts in FAR]
    near, far = len(near_spans), len(far_spans[0])
    part_rows = block // STAGES
    in_hbm = pl.BlockSpec(memory_space=pltpu.HBM)

    dma = pltpu.SemaphoreType.DMA

    return pl.pallas_call(
        functools.partial(kernel, near_spans, far_spans),
        out_shape=pltpu.VMEM((block, out_width), BF16),
        in_specs=[in_hbm] * 6,
        out_specs=pl.BlockSpec(memory_space=pltpu.VMEM),
        scratch_shapes=[
            pltpu.SMEM((blocks,), jnp.int32),
            pltpu.SMEM((blocks,), jnp.int32),
            pltpu.VMEM((rows, depth), BF16),
            pltpu.VMEM((rows, depth), BF16),
            pltpu.VMEM((depth, cols), BF16),
            pltpu.VMEM((count, ranks, depth), BF16),
            pltpu.VMEM((held, ranks, out_width), BF16),
            pltpu.VMEM((8, 128), F32),
            pltpu.VMEM((8, 128), F32),
            pltpu.VMEM((ranks, out_width), BF16),
            pltpu.VMEM((ranks, cols), BF16),
            pltpu.VMEM((ranks, cols), BF16),
            pltpu.VMEM((ranks, cols), BF16),
            pltpu.VMEM((ranks, block), F32),
            pltpu.VMEM((3, ranks, block), F32),
            pltpu.VMEM((3, ranks, block), F32),
            pltpu.VMEM((ranks, block), BF16),
            pltpu.VMEM((ranks, block), BF16),
            pltpu.VMEM((block, cols), F32),
            pltpu.VMEM((block, cols), F32),
            pltpu.VMEM((2, block, cols), PAIR),
            pltpu.VMEM((2, block, cols), PAIR),
            pltpu.VMEM((2, block, cols), F32),
            pltpu.VMEM((STAGES, 2 * part_rows, cols), PAIR),
            pltpu.VMEM((STAGES, 2 * part_rows, cols), PAIR),
            pltpu.VMEM((STAGES, 2 * part_rows, cols), F32),
            pltpu.VMEM((block, cols), BF16),
            pltpu.VMEM((block, cols), BF16),
            pltpu.VMEM((STAGES, part_rows, cols), BF16),
            pltpu.VMEM((STAGES, part_rows, cols), BF16),
            pltpu.VMEM((STAGES, part_rows, cols), BF16),
            pltpu.VMEM((STAGES, part_rows, cols), BF16),
            dma((4,)),
            dma,
            dma((far,)),
        ],
        compiler_params=pltpu.CompilerParams(
            collective_id=0, has_side_effects=True, vmem_limit_bytes=56 * 1024 * 1024
        ),
    )(
        block_adapter_index,
        request_rows,
        tokens,
        base_up_weight,
        adapter_down_weight,
        adapter_up_weight,
    )


def solution(mesh):
    in_specs = (
        P("gx", "gy"),
        P("gy", ("gz", "gx")),
        P(None, None, "gy"),
        P("gx", None, "gz"),
        P("gx"),
        P("gx"),
    )
    out_specs = P(("gx", "gy"), "gz")
    sizes = mesh.shape

    def body(*arrays):
        blocks = arrays[4].shape[0]
        paired = sizes["gx"] == 2 and sizes["gy"] == 4 and sizes["gz"] % 2 == 0
        cols = arrays[1].shape[1]
        cut = cols % (sum(NEAR) * 128) == 0
        cut = cut and arrays[0].shape[0] // blocks % (STAGES * 16) == 0
        if paired and cut and blocks == sizes["gy"]:
            return fused_body(*arrays)
        return general_body(*arrays)

    return jax.shard_map(body, mesh=mesh, in_specs=in_specs, out_specs=out_specs, check_vma=False)
```
